512 devices in a mesh: segment: 16 (over z_hi, y, core), dp: 32 (over x, z_lo).
Axes of the slice: x: 4, y: 4, z: 16 (z_hi: 2, z_lo: 8; z = z_hi * 8 + z_lo), core: 2. Of those that a mesh axis runs over, the one named last changes fastest.
Arguments:
- token_ids: int32 [4096], P('dp'), may hold values from 0 to 152063, as said below
- table: bfloat16 [19008, 28672], P('segment', 'dp'), may hold values from -6 to 6
- out_grad: bfloat16 [4096, 3584], P('dp', 'segment'), may hold values from -6 to 6
Outputs:
- embedded: bfloat16 [4096, 3584], P('dp')
- table_grad: bfloat16 [19008, 28672], P('segment', 'dp')
The draws below stay inside these ranges and needn't reach their ends.
Inputs may be any that keep to these rules, and one draw needn't show every extreme that they name: `token_ids`: in the 128 tokens of each data group, at most 16 ids lie in one segment's slice of 9504 rows with one residue modulo 8; in every data group some segment and residue has exactly 16.
All inputs are finite; a program needn't handle non-finite values.
Results may differ from the reference program's by a relative error of at most 0.001.
Values may be sent and summed in bfloat16 or wider, within the bound.
No kernel may reach another device: no remote copies, remote signals or barrier semaphores. Data moves between devices by JAX's collectives and lax.ppermute only.
A program may use at most 64 MiB of HBM per device.

```python
import jax
import jax.numpy as jnp
from jax import lax

D = 3584
ROWS_SECTION = 9504
PACK = 8
TOK_DEV = 128
VOCAB = 152064
TOKENS = 4096


def draw_token_ids(key, part):
    groups = TOKENS // TOK_DEV
    segments = VOCAB // ROWS_SECTION
    buckets = segments * PACK
    capacity = TOK_DEV // PACK
    lines = ROWS_SECTION // PACK
    global_hot = jax.random.randint(jax.random.fold_in(key, 11), (), 0, buckets)

    def one_group(group):
        group_key = jax.random.fold_in(key, 100 + group)
        keys = jax.random.split(group_key, 7)
        order = jax.random.permutation(keys[0], buckets)
        use_global = jax.random.randint(keys[1], (), 0, 2)
        hot = jnp.where(use_global == 1, global_hot, order[0])
        hot_pos = jnp.argmax(order == hot)
        order = order.at[hot_pos].set(order[0]).at[0].set(hot)
        spread = jax.random.randint(keys[2], (), 7, buckets)
        position = jnp.arange(TOK_DEV)
        bucket = jnp.where(position < capacity, order[0], order[1 + (position - capacity) % spread])
        hot_line = jax.random.randint(keys[3], (TOK_DEV,), 0, min(lines, 4))
        any_line = jax.random.randint(keys[4], (TOK_DEV,), 0, lines)
        pick = jax.random.randint(keys[5], (TOK_DEV,), 0, 2)
        line = jnp.where(pick == 1, hot_line, any_line)
        ids = bucket // PACK * ROWS_SECTION + line * PACK + bucket % PACK
        shuffle = jax.random.permutation(keys[6], TOK_DEV)
        return ids[shuffle]
    return jax.vmap(one_group)(jnp.arange(groups)).reshape(-1).astype(jnp.int32)


def shard_levels(rng, dims, cuts, least, top_value):
    level = 1.0
    for axis_at, shards_of in cuts:
        draws = jax.random.uniform(jax.random.fold_in(jax.random.fold_in(rng, 6), axis_at), (shards_of,), jnp.float32, least / len(cuts), top_value / len(cuts))
        level = level * jnp.repeat(jnp.exp(draws), dims[axis_at] // shards_of).reshape((-1,) + (1,) * (len(dims) - 1 - axis_at))
    return level


def normal_values(own_key, shape, deviation, most, cuts=(), held_as=jnp.bfloat16):
    drawn = jax.random.normal(own_key, shape, jnp.float32) * deviation
    if len(cuts) > 0:
        drawn = shard_levels(own_key, shape, cuts, -0.22, 0.18) * drawn
    return jnp.clip(drawn, min=-most, max=most).astype(held_as)


def setup_inputs(seed: int = 0) -> dict:
    splits = jax.random.split(jax.random.key(seed), 4)
    token_ids = draw_token_ids(jax.random.fold_in(splits[3], 71), 0)
    table = normal_values(splits[1], (VOCAB // PACK, PACK * D), 1.0, 6.0, ((0, 16), (1, 32)))
    out_grad = normal_values(splits[2], (TOKENS, D), 1.0, 6.0, ((0, 32), (1, 16)))
    return {"token_ids": token_ids, "table": table, "out_grad": out_grad}


def reference(token_ids, table, out_grad):
    flat = table.reshape(VOCAB, D)
    embedded = jnp.take(flat, token_ids, axis=0)
    width = 128 if D % 128 == 0 else D
    blocks = D // width
    pieces = out_grad.reshape(TOKENS, blocks, width).transpose(1, 0, 2)

    def accumulate(piece):
        total = jnp.zeros((VOCAB, width), jnp.float32).at[token_ids].add(piece.astype(jnp.float32))
        return total.astype(jnp.bfloat16)

    summed = lax.map(accumulate, pieces)
    table_grad = summed.transpose(1, 0, 2).reshape(VOCAB // PACK, PACK * D)
    return embedded, table_grad
```

```python
import itertools

import jax
import jax.numpy as jnp
from jax import lax
from jax.sharding import Mesh, PartitionSpec as P

D = 3584
PACK = 8
SLOTS = 16
NAMES = ("z_hi", "y", "core", "x", "z_lo")
SIZES = (2, 4, 2, 4, 8)
PLANE = ("y", "core", "x")
GROUPS = ("x", "z_lo")
QUARTERS = 4
WIDTH = D // QUARTERS
BF16 = jnp.bfloat16


def move(values, to):
    def flat(place):
        number = 0
        for size, at in zip(SIZES, place):
            number = number * size + at
        return number

    pairs = [
        (flat(place), flat(to(*place)))
        for place in itertools.product(*(range(size) for size in SIZES))
    ]
    return lax.ppermute(values, NAMES, pairs)


def lookup_code(z_hi, z_lo):
    return z_lo


def grad_code(z_hi, z_lo):
    return z_hi * 4 + (z_lo // 4) * 2 + z_lo % 2


def grad_target(z_hi, y, core, x, z_lo):
    code = (core * 4 + y) ^ z_lo
    return (code // 4, y, core, x, ((code // 2) % 2) * 4 + 2 * z_hi + code % 2)


def groups_of_plane(code):
    at = jnp.arange(32, dtype=jnp.int32)
    y, core, x = at // 8, (at // 4) % 2, at % 4
    return x * 8 + ((core * 4 + y) ^ code)


def pick_matrix(ids, section, z_hi, parity):
    segment = ids // section
    residue = (ids % section) % PACK
    bucket = segment * PACK + residue
    count = ids.shape[0]
    order = jnp.arange(count, dtype=jnp.int32)
    earlier = (bucket[:, None] == bucket[None, :]) & (order[None, :] < order[:, None])
    rank = jnp.sum(earlier.astype(jnp.int32), axis=1)
    here = (segment // 8 == z_hi) & (residue % 2 == parity)
    slot = jnp.where(here, ((segment % 8) * 4 + residue // 2) * SLOTS + rank, -1)
    return (slot[:, None] == jnp.arange(32 * SLOTS, dtype=jnp.int32)[None, :]).astype(BF16)


def body(token_ids, table, out_grad):
    lines, width = table.shape
    section = lines * PACK
    tokens = token_ids.shape[0]
    z_hi, y, core, x, z_lo = (lax.axis_index(name) for name in NAMES)
    segment = (z_hi * 4 + y) * 2 + core
    residue = x * 2 + z_lo // 4
    parity = z_lo // 4
    place = core * 4 + y

    every_id = lax.all_to_all(
        jnp.broadcast_to(token_ids[None], (32, tokens)), GROUPS, 0, 0, tiled=True
    )

    code_f = lookup_code(z_hi, z_lo)
    code_b = grad_code(z_hi, z_lo)
    orders = jnp.concatenate([groups_of_plane(code_f), groups_of_plane(code_b)])
    ids = jnp.take(every_id, orders, axis=0)
    local = ids - segment * section
    owned = (local >= 0) & (local < section) & (local % PACK == residue)
    line = local // PACK
    steps = jnp.arange(tokens, dtype=jnp.int32)
    before = (steps[:, None] < steps[None, :]).astype(BF16)
    rank = jnp.dot(owned.astype(BF16), before, preferred_element_type=jnp.float32).astype(jnp.int32)
    slots = jnp.arange(SLOTS, dtype=jnp.int32)
    hit = owned[:, None, :] & (rank[:, None, :] == slots[None, :, None])
    row_of = jnp.sum(jnp.where(hit, line[:, None, :] + 1, 0), axis=2) - 1

    fetched = jnp.take(table, jnp.maximum(row_of[:32], 0).reshape(-1), axis=0)
    arrived = lax.all_to_all(fetched.reshape(32, SLOTS, width), PLANE, 0, 0, tiled=True)
    ids_f = lax.dynamic_index_in_dim(every_id, x * 8 + (place ^ code_f), 0, keepdims=False)
    pick_f = pick_matrix(ids_f, section, z_hi, parity)
    picked = jnp.dot(
        pick_f, arrived.reshape(32 * SLOTS, width), preferred_element_type=jnp.float32
    ).astype(BF16)

    def near(a, b, c, d, e):
        return (a, b, c, d, e ^ (c * 4 + b))

    def far(a, b, c, d, e):
        return (1 - a, b, c, d, e ^ (c * 4 + b))

    both = move(picked, near) + move(picked, far)
    quarter = both + lax.ppermute(both, "core", [(0, 1), (1, 0)])
    whole = lax.all_gather(quarter, "y")
    embedded = jnp.concatenate(
        [
            lax.dynamic_index_in_dim(whole, (z_lo % 4) ^ part, 0, keepdims=False)
            for part in range(QUARTERS)
        ],
        axis=1,
    )

    halves = lax.all_gather(out_grad, ("y", "core"), axis=1, tiled=True)
    which = (place ^ z_lo) % 2
    piece = lax.dynamic_slice(halves, (0, which * width), (tokens, width))
    piece = move(piece, grad_target)
    ids_b = lax.dynamic_index_in_dim(every_id, x * 8 + (place ^ code_b), 0, keepdims=False)
    pick_b = pick_matrix(ids_b, section, z_hi, parity)
    packed = lax.dot_general(
        pick_b, piece, (((0,), (0,)), ((), ())), preferred_element_type=jnp.float32
    ).astype(BF16)
    returned = lax.all_to_all(packed.reshape(32, SLOTS, width), PLANE, 0, 0, tiled=True)
    target = row_of[32:].reshape(-1)
    spread = (jnp.arange(lines, dtype=jnp.int32)[:, None] == target[None, :]).astype(BF16)
    table_grad = jnp.dot(
        spread, returned.reshape(32 * SLOTS, width), preferred_element_type=jnp.float32
    ).astype(BF16)
    return embedded, table_grad


def solution(mesh):
    fine = Mesh(mesh.devices.reshape(SIZES), NAMES)
    segment, groups = ("z_hi", "y", "core"), ("x", "z_lo")
    return jax.shard_map(
        body,
        mesh=fine,
        in_specs=(P(groups), P(segment, groups), P(groups, segment)),
        out_specs=(P(groups, None), P(segment, groups)),
        check_vma=False,
    )
```

```python
import itertools

import jax
import jax.numpy as jnp
from jax import lax
from jax.sharding import Mesh, PartitionSpec as P


PACK = 8
SLOTS = 16
NAMES = ("z_hi", "y", "core", "x", "z_lo")
SIZES = (2, 4, 2, 4, 8)
PLANE = ("y", "core", "x")
GROUPS = ("x", "z_lo")
QUARTERS = 4
BF16 = jnp.bfloat16


def move(values, to):
    def flat(place):
        number = 0
        for size, at in zip(SIZES, place):
            number = number * size + at
        return number

    pairs = [
        (flat(place), flat(to(*place)))
        for place in itertools.product(*(range(size) for size in SIZES))
    ]
    return lax.ppermute(values, NAMES, pairs)


def grad_code(z_hi, z_lo):
    return z_hi * 4 + (z_lo // 4) * 2 + z_lo % 2


def grad_target(z_hi, y, core, x, z_lo):
    code = (core * 4 + y) ^ z_lo
    return (code // 4, y, core, x, ((code // 2) % 2) * 4 + 2 * z_hi + code % 2)


def groups_of_plane(code):
    at = jnp.arange(32, dtype=jnp.int32)
    y, core, x = at // 8, (at // 4) % 2, at % 4
    return x * 8 + ((core * 4 + y) ^ code)


def pick_matrix(ids, section, z_hi, parity):
    segment = ids // section
    residue = (ids % section) % PACK
    bucket = segment * PACK + residue
    count = ids.shape[0]
    order = jnp.arange(count, dtype=jnp.int32)
    earlier = (bucket[:, None] == bucket[None, :]) & (order[None, :] < order[:, None])
    rank = jnp.sum(earlier.astype(jnp.int32), axis=1)
    here = (segment // 8 == z_hi) & (residue % 2 == parity)
    slot = jnp.where(here, ((segment % 8) * 4 + residue // 2) * SLOTS + rank, -1)
    return (slot[:, None] == jnp.arange(32 * SLOTS, dtype=jnp.int32)[None, :]).astype(BF16)


def body(token_ids, table, out_grad):
    lines, width = table.shape
    section = lines * PACK
    tokens = token_ids.shape[0]
    z_hi, y, core, x, z_lo = (lax.axis_index(name) for name in NAMES)
    segment = (z_hi * 4 + y) * 2 + core
    residue = x * 2 + z_lo // 4
    parity = z_lo // 4
    place = core * 4 + y

    every_id = lax.all_to_all(
        jnp.broadcast_to(token_ids[None], (32, tokens)), GROUPS, 0, 0, tiled=True
    )
    halves = lax.all_gather(out_grad, ("y", "core"), axis=1, tiled=True)
    every_id, halves = lax.optimization_barrier((every_id, halves))
    which = (place ^ z_lo) % 2
    piece = lax.dynamic_slice(halves, (0, which * width), (tokens, width))
    piece = move(piece, grad_target)

    code_f = z_lo
    code_b = grad_code(z_hi, z_lo)
    orders = jnp.concatenate([groups_of_plane(code_f), groups_of_plane(code_b)])
    ids = jnp.take(every_id, orders, axis=0, mode="clip")
    local = ids - segment * section
    owned = (local >= 0) & (local < section) & (local % PACK == residue)
    line = local // PACK
    steps = jnp.arange(tokens, dtype=jnp.int32)
    before = (steps[:, None] < steps[None, :]).astype(BF16)
    rank = jnp.dot(owned.astype(BF16), before, preferred_element_type=jnp.float32).astype(jnp.int32)
    slots = jnp.arange(SLOTS, dtype=jnp.int32)
    hit = owned[:, None, :] & (rank[:, None, :] == slots[None, :, None])
    row_of = jnp.sum(jnp.where(hit, line[:, None, :] + 1, 0), axis=2) - 1

    fetched = jnp.take(table, jnp.maximum(row_of[:32], 0).reshape(-1), axis=0, mode="clip")
    arrived = lax.all_to_all(fetched.reshape(32, SLOTS, width), PLANE, 0, 0, tiled=True)
    ids_f = lax.dynamic_index_in_dim(every_id, x * 8 + (place ^ code_f), 0, keepdims=False)
    pick_f = pick_matrix(ids_f, section, z_hi, parity)
    picked = jnp.dot(
        pick_f, arrived.reshape(32 * SLOTS, width), preferred_element_type=jnp.float32
    ).astype(BF16)

    def near(a, b, c, d, e):
        return (a, b, c, d, e ^ (c * 4 + b))

    def far(a, b, c, d, e):
        return (1 - a, b, c, d, e ^ (c * 4 + b))

    both = move(picked, near) + move(picked, far)
    quarter = both + lax.ppermute(both, "core", [(0, 1), (1, 0)])
    whole = lax.all_gather(quarter, "y")
    embedded = jnp.concatenate(
        [
            lax.dynamic_index_in_dim(whole, (z_lo % 4) ^ part, 0, keepdims=False)
            for part in range(QUARTERS)
        ],
        axis=1,
    )

    ids_b = lax.dynamic_index_in_dim(every_id, x * 8 + (place ^ code_b), 0, keepdims=False)
    pick_b = pick_matrix(ids_b, section, z_hi, parity)
    packed = lax.dot_general(
        pick_b, piece, (((0,), (0,)), ((), ())), preferred_element_type=jnp.float32
    ).astype(BF16)
    returned = lax.all_to_all(packed.reshape(32, SLOTS, width), PLANE, 0, 0, tiled=True)
    target = row_of[32:].reshape(-1)
    spread = (jnp.arange(lines, dtype=jnp.int32)[:, None] == target[None, :]).astype(BF16)
    table_grad = jnp.dot(
        spread, returned.reshape(32 * SLOTS, width), preferred_element_type=jnp.float32
    ).astype(BF16)
    return embedded, table_grad


def solution(mesh):
    fine = Mesh(mesh.devices.reshape(SIZES), NAMES)
    segment, groups = ("z_hi", "y", "core"), ("x", "z_lo")

    return jax.shard_map(
        body,
        mesh=fine,
        in_specs=(P(groups), P(segment, groups), P(groups, segment)),
        out_specs=(P(groups, None), P(segment, groups)),
        check_vma=False,
    )
```

```python
import functools
import itertools

import jax
import jax.numpy as jnp
from jax import lax
from jax.sharding import Mesh, PartitionSpec as P


PACK = 8
SLOTS = 16
NAMES = ("z_hi", "y", "core", "x", "z_lo")
SIZES = (2, 4, 2, 4, 8)
PLANE = ("y", "core", "x")
GROUPS = ("x", "z_lo")
QUARTERS = 4
BF16 = jnp.bfloat16


def move(values, to):
    def flat(place):
        number = 0
        for size, at in zip(SIZES, place):
            number = number * size + at
        return number

    pairs = [
        (flat(place), flat(to(*place)))
        for place in itertools.product(*(range(size) for size in SIZES))
    ]
    return lax.ppermute(values, NAMES, pairs)


def grad_code(z_hi, z_lo):
    return z_hi * 4 + (z_lo // 4) * 2 + z_lo % 2


def grad_target(k, z_hi, y, core, x, z_lo):
    high, low = y // 2, y % 2
    parity = k ^ low ^ ((z_lo // 2) % 2)
    return (
        core ^ (z_lo // 4),
        2 * (k ^ low) + ((z_lo % 2) ^ high),
        core,
        x,
        parity * 4 + 2 * z_hi + high,
    )


def groups_of_plane(code):
    at = jnp.arange(32, dtype=jnp.int32)
    y, core, x = at // 8, (at // 4) % 2, at % 4
    return x * 8 + ((core * 4 + y) ^ code)


def pick_matrix(ids, section, z_hi, parity):
    segment = ids // section
    residue = (ids % section) % PACK
    bucket = segment * PACK + residue
    count = ids.shape[0]
    order = jnp.arange(count, dtype=jnp.int32)
    earlier = (bucket[:, None] == bucket[None, :]) & (order[None, :] < order[:, None])
    rank = jnp.sum(earlier.astype(jnp.int32), axis=1)
    here = (segment // 8 == z_hi) & (residue % 2 == parity)
    slot = jnp.where(here, ((segment % 8) * 4 + residue // 2) * SLOTS + rank, -1)
    return (slot[:, None] == jnp.arange(32 * SLOTS, dtype=jnp.int32)[None, :]).astype(BF16)


def body(token_ids, table, out_grad):
    lines, width = table.shape
    section = lines * PACK
    tokens = token_ids.shape[0]
    z_hi, y, core, x, z_lo = (lax.axis_index(name) for name in NAMES)
    segment = (z_hi * 4 + y) * 2 + core
    residue = x * 2 + z_lo // 4
    parity = z_lo // 4
    place = core * 4 + y

    every_id = lax.all_to_all(
        jnp.broadcast_to(token_ids[None], (32, tokens)), GROUPS, 0, 0, tiled=True
    )
    own = out_grad.T
    other = move(own, lambda a, b, c, d, e: (a, b, 1 - c, d, e))
    half = jnp.concatenate(
        [jnp.where(core == 0, own, other), jnp.where(core == 0, other, own)]
    )
    early = move(half, functools.partial(grad_target, 0))
    late = move(half, functools.partial(grad_target, 1))
    sent = (early, late)

    code_f = z_lo
    code_b = grad_code(z_hi, z_lo)
    orders = jnp.concatenate([groups_of_plane(code_f), groups_of_plane(code_b)])
    ids = jnp.take(every_id, orders, axis=0, mode="clip")
    local = ids - segment * section
    owned = (local >= 0) & (local < section) & (local % PACK == residue)
    line = local // PACK
    steps = jnp.arange(tokens, dtype=jnp.int32)
    before = (steps[:, None] < steps[None, :]).astype(BF16)
    rank = jnp.dot(owned.astype(BF16), before, preferred_element_type=jnp.float32).astype(jnp.int32)
    slots = jnp.arange(SLOTS, dtype=jnp.int32)
    hit = owned[:, None, :] & (rank[:, None, :] == slots[None, :, None])
    row_of = jnp.sum(jnp.where(hit, line[:, None, :] + 1, 0), axis=2) - 1

    fetched = jnp.take(table, jnp.maximum(row_of[:32], 0).reshape(-1), axis=0, mode="clip")
    arrived = lax.all_to_all(fetched.reshape(32, SLOTS, width), PLANE, 0, 0, tiled=True)
    ids_f = lax.dynamic_index_in_dim(every_id, x * 8 + (place ^ code_f), 0, keepdims=False)
    pick_f = pick_matrix(ids_f, section, z_hi, parity)
    picked = jnp.dot(
        pick_f, arrived.reshape(32 * SLOTS, width), preferred_element_type=jnp.float32
    ).astype(BF16)

    def near(a, b, c, d, e):
        return (a, b, c, d, e ^ (c * 4 + b))

    def far(a, b, c, d, e):
        return (1 - a, b, c, d, e ^ (c * 4 + b))

    both = move(picked, near) + move(picked, far)
    quarter = both + lax.ppermute(both, "core", [(0, 1), (1, 0)])
    whole = lax.all_gather(quarter, "y")
    embedded = jnp.concatenate(
        [
            lax.dynamic_index_in_dim(whole, (z_lo % 4) ^ part, 0, keepdims=False)
            for part in range(QUARTERS)
        ],
        axis=1,
    )

    ids_b = lax.dynamic_index_in_dim(every_id, x * 8 + (place ^ code_b), 0, keepdims=False)
    pick_b = pick_matrix(ids_b, section, z_hi, parity)
    swapped = y // 2 == 1
    piece = jnp.concatenate(
        [jnp.where(swapped, sent[1], sent[0]), jnp.where(swapped, sent[0], sent[1])]
    )
    packed = lax.dot_general(
        pick_b, piece, (((0,), (1,)), ((), ())), preferred_element_type=jnp.float32
    ).astype(BF16)
    returned = lax.all_to_all(packed.reshape(32, SLOTS, width), PLANE, 0, 0, tiled=True)
    target = row_of[32:].reshape(-1)
    spread = (jnp.arange(lines, dtype=jnp.int32)[:, None] == target[None, :]).astype(BF16)
    table_grad = jnp.dot(
        spread, returned.reshape(32 * SLOTS, width), preferred_element_type=jnp.float32
    ).astype(BF16)
    return embedded, table_grad


def solution(mesh):
    fine = Mesh(mesh.devices.reshape(SIZES), NAMES)
    segment, groups = ("z_hi", "y", "core"), ("x", "z_lo")

    return jax.shard_map(
        body,
        mesh=fine,
        in_specs=(P(groups), P(segment, groups), P(groups, segment)),
        out_specs=(P(groups, None), P(segment, groups)),
        check_vma=False,
    )
```

```python
import functools
import itertools

import jax
import jax.numpy as jnp
from jax import lax
from jax.sharding import Mesh, PartitionSpec as P


PACK = 8
SLOTS = 16
NAMES = ("z_hi", "y", "core", "x", "z_lo")
SIZES = (2, 4, 2, 4, 8)
PLANE = ("y", "core", "x")
GROUPS = ("x", "z_lo")
QUARTERS = 4
BF16 = jnp.bfloat16


def move(values, to):
    def flat(place):
        number = 0
        for size, at in zip(SIZES, place):
            number = number * size + at
        return number

    pairs = [
        (flat(place), flat(to(*place)))
        for place in itertools.product(*(range(size) for size in SIZES))
    ]
    return lax.ppermute(values, NAMES, pairs)


def lookup_code(z_hi, z_lo):
    return z_lo ^ (z_hi * 4)


def grad_code(z_hi, z_lo):
    return z_hi * 4 + (z_lo // 4) * 2 + z_lo % 2


def grad_target(k, z_hi, y, core, x, z_lo):
    high, low = y // 2, y % 2
    parity = k ^ low ^ ((z_lo // 2) % 2)
    return (
        core ^ (z_lo // 4),
        2 * (k ^ low) + ((z_lo % 2) ^ high),
        core,
        x,
        parity * 4 + 2 * z_hi + high,
    )


def groups_of_plane(code):
    at = jnp.arange(32, dtype=jnp.int32)
    y, core, x = at // 8, (at // 4) % 2, at % 4
    return x * 8 + ((core * 4 + y) ^ code)


def pick_matrix(ids, section, z_hi, parity):
    segment = ids // section
    residue = (ids % section) % PACK
    bucket = segment * PACK + residue
    count = ids.shape[0]
    order = jnp.arange(count, dtype=jnp.int32)
    earlier = (bucket[:, None] == bucket[None, :]) & (order[None, :] < order[:, None])
    rank = jnp.sum(earlier.astype(jnp.int32), axis=1)
    here = (segment // 8 == z_hi) & (residue % 2 == parity)
    slot = jnp.where(here, ((segment % 8) * 4 + residue // 2) * SLOTS + rank, -1)
    return (slot[:, None] == jnp.arange(32 * SLOTS, dtype=jnp.int32)[None, :]).astype(BF16)


def body(token_ids, table, out_grad):
    lines, width = table.shape
    section = lines * PACK
    tokens = token_ids.shape[0]
    z_hi, y, core, x, z_lo = (lax.axis_index(name) for name in NAMES)
    segment = (z_hi * 4 + y) * 2 + core
    residue = x * 2 + z_lo // 4
    parity = z_lo // 4
    place = core * 4 + y

    every_id = lax.all_to_all(
        jnp.broadcast_to(token_ids[None], (32, tokens)), GROUPS, 0, 0, tiled=True
    )
    own = out_grad.T
    other = move(own, lambda a, b, c, d, e: (a, b, 1 - c, d, e))
    half = jnp.concatenate(
        [jnp.where(core == 0, own, other), jnp.where(core == 0, other, own)]
    )
    early = move(half, functools.partial(grad_target, 0))
    late = move(half, functools.partial(grad_target, 1))
    sent = (early, late)

    code_f = lookup_code(z_hi, z_lo)
    code_b = grad_code(z_hi, z_lo)
    ids = jnp.take(every_id, groups_of_plane(code_f), axis=0, mode="clip")
    local = ids - segment * section
    owned = (local >= 0) & (local < section) & (local % PACK == residue)
    line = local // PACK
    steps = jnp.arange(tokens, dtype=jnp.int32)
    before = (steps[:, None] < steps[None, :]).astype(BF16)
    rank = jnp.dot(owned.astype(BF16), before, preferred_element_type=jnp.float32).astype(jnp.int32)
    slots = jnp.arange(SLOTS, dtype=jnp.int32)
    hit = owned[:, None, :] & (rank[:, None, :] == slots[None, :, None])
    row_of = jnp.sum(jnp.where(hit, line[:, None, :] + 1, 0), axis=2) - 1

    fetched = jnp.take(table, jnp.maximum(row_of, 0).reshape(-1), axis=0, mode="clip")
    arrived = lax.all_to_all(fetched.reshape(32, SLOTS, width), PLANE, 0, 0, tiled=True)
    ids_f = lax.dynamic_index_in_dim(every_id, x * 8 + (place ^ code_f), 0, keepdims=False)
    pick_f = pick_matrix(ids_f, section, z_hi, parity)
    picked = jnp.dot(
        pick_f, arrived.reshape(32 * SLOTS, width), preferred_element_type=jnp.float32
    ).astype(BF16)

    def near(a, b, c, d, e):
        return (a, b, c, d, lookup_code(a, e) ^ (c * 4 + b))

    def far(a, b, c, d, e):
        return (1 - a, b, c, d, lookup_code(a, e) ^ (c * 4 + b))

    both = move(picked, near) + move(picked, far)
    quarter = both + lax.ppermute(both, "core", [(0, 1), (1, 0)])
    whole = lax.all_gather(quarter, "y")
    embedded = jnp.concatenate(
        [
            lax.dynamic_index_in_dim(whole, (z_lo % 4) ^ part, 0, keepdims=False)
            for part in range(QUARTERS)
        ],
        axis=1,
    )

    ids_b = lax.dynamic_index_in_dim(every_id, x * 8 + (place ^ code_b), 0, keepdims=False)
    pick_b = pick_matrix(ids_b, section, z_hi, parity)
    swapped = y // 2 == 1
    piece = jnp.concatenate(
        [jnp.where(swapped, sent[1], sent[0]), jnp.where(swapped, sent[0], sent[1])]
    )
    packed = lax.dot_general(
        pick_b, piece, (((0,), (1,)), ((), ())), preferred_element_type=jnp.float32
    ).astype(BF16)
    late_id, packed = lax.optimization_barrier((every_id.reshape(-1), packed))
    returned = lax.all_to_all(packed.reshape(32, SLOTS, width), PLANE, 0, 0, tiled=True)
    late_local = late_id - segment * section
    late_owned = (late_local >= 0) & (late_local < section) & (late_local % PACK == residue)
    late_line = jnp.where(late_owned, late_local // PACK + 1, 0).reshape(32, tokens)
    late_line = jnp.take(late_line, groups_of_plane(code_b), axis=0, mode="clip")
    late_rank = jnp.dot(
        (late_line > 0).astype(BF16), before, preferred_element_type=jnp.float32
    ).astype(jnp.int32)
    late_hit = late_rank[:, None, :] == slots[None, :, None]
    target = jnp.sum(jnp.where(late_hit, late_line[:, None, :], 0), axis=2).reshape(-1) - 1
    spread = (jnp.arange(lines, dtype=jnp.int32)[:, None] == target[None, :]).astype(BF16)
    table_grad = jnp.dot(
        spread, returned.reshape(32 * SLOTS, width), preferred_element_type=jnp.float32
    ).astype(BF16)
    return embedded, table_grad


def solution(mesh):
    fine = Mesh(mesh.devices.reshape(SIZES), NAMES)
    segment, groups = ("z_hi", "y", "core"), ("x", "z_lo")

    return jax.shard_map(
        body,
        mesh=fine,
        in_specs=(P(groups), P(segment, groups), P(groups, segment)),
        out_specs=(P(groups, None), P(segment, groups)),
        check_vma=False,
    )
```
